128 devices in a mesh: tp: 4 (over x), dp: 32 (over z, y, core).
Axes of the slice: x: 4, y: 4, z: 4, core: 2. Of those that a mesh axis runs over, the one named last changes fastest.
Arguments:
- feat_in: bfloat16 [32768, 1728], P('dp', 'tp')
- grad_out: float32 [32768, 512], P('dp')
- w_down: bfloat16 [3, 4, 1728, 512], P(None, None, 'tp')
- w_core: bfloat16 [3, 4, 512, 512], replicated
- w_up: bfloat16 [3, 4, 512, 1728], P(None, None, None, 'tp')
- w_gate: bfloat16 [3, 1728, 4], P(None, 'tp')
- bias_cross: bfloat16 [3, 1728], P(None, 'tp')
- w_top: bfloat16 [1728, 512], P('tp')
Outputs:
- output 1: float32 [32768, 512], P('dp')
- output 2: float32 [32768, 1728], P('dp', 'tp')
- output 3: float32 [3, 4, 1728, 512], P(None, None, 'tp')
- output 4: float32 [3, 4, 512, 512], replicated
- output 5: float32 [3, 4, 512, 1728], P(None, None, None, 'tp')
- output 6: float32 [3, 1728, 4], P(None, 'tp')
- output 7: float32 [3, 1728], P(None, 'tp')
- output 8: float32 [1728, 512], P('tp')
All inputs are finite; a program needn't handle non-finite values.
Results may differ from the reference program's by a relative error of at most 0.0126463.
Values sent between devices are 32-bit elements.
A program may use at most 1 GiB of HBM per device.

```python
import jax
import jax.numpy as jnp
from jax import lax

FEAT_WIDTH = 1728
LOW_RANK = 512
NUM_EXPERTS = 4
NUM_LAYERS = 3
TOP_WIDTH = 512
BATCH_ROWS = 32768
BLOCK_ROWS = 1024


def setup_inputs(seed: int = 0) -> dict:
    keys = jax.random.split(jax.random.key(seed), 8)
    feat_in = jax.random.normal(keys[0], (BATCH_ROWS, FEAT_WIDTH), jnp.float32)
    grad_out = jax.random.normal(keys[1], (BATCH_ROWS, TOP_WIDTH), jnp.float32)
    w_down = jax.random.normal(keys[2], (NUM_LAYERS, NUM_EXPERTS, FEAT_WIDTH, LOW_RANK), jnp.float32) * FEAT_WIDTH ** -0.5
    w_core = jax.random.normal(keys[3], (NUM_LAYERS, NUM_EXPERTS, LOW_RANK, LOW_RANK), jnp.float32) * (1.5 * LOW_RANK ** -0.5)
    w_up = jax.random.normal(keys[4], (NUM_LAYERS, NUM_EXPERTS, LOW_RANK, FEAT_WIDTH), jnp.float32) * (1.5 * LOW_RANK ** -0.5)
    w_gate = jax.random.normal(keys[5], (NUM_LAYERS, FEAT_WIDTH, NUM_EXPERTS), jnp.float32) * (2.0 * FEAT_WIDTH ** -0.5)
    bias_cross = jax.random.normal(keys[6], (NUM_LAYERS, FEAT_WIDTH), jnp.float32) * 0.5
    w_top = jax.random.normal(keys[7], (FEAT_WIDTH, TOP_WIDTH), jnp.float32) * FEAT_WIDTH ** -0.5
    return {'feat_in': feat_in.astype(jnp.bfloat16), 'grad_out': grad_out, 'w_down': w_down.astype(jnp.bfloat16), 'w_core': w_core.astype(jnp.bfloat16), 'w_up': w_up.astype(jnp.bfloat16), 'w_gate': w_gate.astype(jnp.bfloat16), 'bias_cross': bias_cross.astype(jnp.bfloat16), 'w_top': w_top.astype(jnp.bfloat16)}


def bf16_value(tensor):
    return tensor + lax.stop_gradient(tensor.astype(jnp.bfloat16).astype(jnp.float32) - tensor)


def cross_forward(params, feat_rows):
    w_down, w_core, w_up, w_gate, bias_cross, w_top = params
    state = feat_rows
    for layer in range(NUM_LAYERS):
        down_proj = jnp.einsum('nw,ewr->ner', state, w_down[layer])
        act_one = jnp.tanh(down_proj)
        act_two = jnp.tanh(jnp.einsum('ner,ers->nes', bf16_value(act_one), w_core[layer]))
        gate = jax.nn.softmax(jnp.dot(state, w_gate[layer]), axis=-1)
        mixed = bf16_value(gate[:, :, None] * act_two)
        mix_out = jnp.einsum('ner,erw->nw', mixed, w_up[layer])
        state = bf16_value(state + feat_rows * (mix_out + bias_cross[layer]))
    return jnp.dot(state, w_top)


def reference(feat_in, grad_out, w_down, w_core, w_up, w_gate, bias_cross, w_top):
    params = tuple(weight.astype(jnp.float32) for weight in (w_down, w_core, w_up, w_gate, bias_cross, w_top))
    block_count = BATCH_ROWS // BLOCK_ROWS
    feat_blocks = feat_in.astype(jnp.float32).reshape(block_count, BLOCK_ROWS, FEAT_WIDTH)
    grad_blocks = grad_out.astype(jnp.float32).reshape(block_count, BLOCK_ROWS, TOP_WIDTH)
    zero_grads = tuple(jnp.zeros_like(weight) for weight in params)

    def block_step(carry, block):
        feat_rows, grad_rows = block
        top_rows, pull_back = jax.vjp(cross_forward, params, feat_rows)
        param_grads, feat_grad = pull_back(grad_rows)
        carry = tuple(total + part for total, part in zip(carry, param_grads))
        return carry, (top_rows, feat_grad)

    totals, (top_blocks, feat_grad_blocks) = lax.scan(block_step, zero_grads, (feat_blocks, grad_blocks))
    return (top_blocks.reshape(BATCH_ROWS, TOP_WIDTH), feat_grad_blocks.reshape(BATCH_ROWS, FEAT_WIDTH), totals[0], totals[1], totals[2], totals[3], totals[4], totals[5])
```

```python
import jax
import jax.numpy as jnp
from jax import lax
from jax.experimental import pallas as pl
from jax.experimental.pallas import tpu as pltpu
from jax.sharding import Mesh, PartitionSpec as P

BF = jnp.bfloat16
F32 = jnp.float32
PLANE = ('z', 'y')
CHIPS = ('tp', 'z', 'y')


def cost(flops, nbytes):
    return pl.CostEstimate(flops=flops, bytes_accessed=nbytes, transcendentals=0)


def unpack_kernel(tiles_ref, out_ref):
    for q in range(tiles_ref.shape[2]):
        out_ref[0, :, q * 128:(q + 1) * 128] = tiles_ref[0, 0, q].astype(BF)


def round_kernel(in_ref, out_ref):
    out_ref[...] = in_ref[...].astype(BF)


def round_low(values):
    return pl.pallas_call(round_kernel, out_shape=jax.ShapeDtypeStruct(values.shape, BF))(values)


def outer_kernel(left_ref, right_ref, out_ref):
    prod = lax.dot_general(left_ref[...], right_ref[0], (((1,), (1,)), ((), ())), preferred_element_type=F32)
    half = out_ref.shape[4]
    for q in range(out_ref.shape[1]):
        for h in range(out_ref.shape[2]):
            out_ref[0, q, h, 0] = prod[h * half:(h + 1) * half, q * 128:(q + 1) * 128]


def place_kernel(core_ref, mine_ref, theirs_ref, *refs):
    down_ref, up_ref = refs[-2:]
    own = (pl.program_id(0) // 2 == core_ref[0])
    half = mine_ref.shape[4]
    for q in range(mine_ref.shape[1]):
        for h in range(mine_ref.shape[2]):
            for kind, out_ref in ((0, up_ref), (1, down_ref)):
                block = jnp.where(own, mine_ref[0, q, h, kind], theirs_ref[0, q, h, kind])
                out_ref[0, 0, h * half:(h + 1) * half, q * 128:(q + 1) * 128] = block


def solution(mesh):
    tp = mesh.shape['tp']
    mesh = Mesh(mesh.devices.reshape(tp, 4, 4, 2), ('tp', 'z', 'y', 'core'))
    plane = 16

    def finite(values):
        return jnp.clip(values, jnp.finfo(F32).min, jnp.finfo(F32).max)

    def mm(spec, a, b):
        return jnp.einsum(spec, a, b, preferred_element_type=F32)

    def swap(values):
        return lax.ppermute(values, 'core', [(0, 1), (1, 0)])

    def flip(values):
        half = values.shape[-1] // 2
        return jnp.concatenate([values[..., half:], values[..., :half]], axis=-1)

    def both(part):
        return part + flip(swap(part))

    def device_body(feat_in, grad_out, w_down, w_core, w_up, w_gate, bias_cross, w_top):
        layers, experts, shard, rank = w_down.shape
        rows = feat_in.shape[0] // tp
        width = shard * tp
        heads = w_top.shape[1]
        own = experts // 2
        t = lax.axis_index('tp')
        core = lax.axis_index('core')
        spot = lax.axis_index('z') * 4 + lax.axis_index('y')
        tiles = rank // 128
        half = shard // 2
        slot, col = spot // tiles, spot % tiles
        first = core * own

        pick = first + slot % own
        up_turned = w_up.transpose(0, 1, 3, 2)
        down_piece = lax.dynamic_slice(w_down, (0, pick, 0, col * 128), (layers, 1, shard, 128))
        up_piece = lax.dynamic_slice(up_turned, (0, pick, 0, col * 128), (layers, 1, shard, 128))
        pieces = finite(jnp.where(slot < own, down_piece, up_piece).astype(F32))[:, 0]
        gathered = [lax.all_gather(pieces[layer], CHIPS, axis=0) for layer in range(layers)]
        top_len = shard // plane
        top_piece = lax.dynamic_slice(w_top, (spot * top_len, 0), (top_len, heads)).astype(F32)
        top_piece = finite(jnp.pad(top_piece, ((0, -top_len % 8), (0, 0))))
        top_all = lax.all_gather(top_piece, CHIPS, axis=0)

        send = finite(feat_in.T.astype(F32)).reshape(shard, tp, rows).transpose(1, 0, 2)
        got = lax.all_to_all(send, 'tp', 0, 0).reshape(width, rows)
        feat = jnp.concatenate([got, swap(got)], axis=1)
        small = jnp.concatenate([w_gate.transpose(0, 2, 1), bias_cross[:, None, :]], axis=1)
        small = finite(small.reshape(layers * (experts + 1), shard).astype(F32))
        small = lax.all_gather(small, 'tp', axis=0).transpose(1, 0, 2).reshape(layers, experts + 1, width)
        gate_w = small[:, :experts].astype(BF)
        bias = small[:, experts]
        own_gate = lax.dynamic_slice(gate_w, (0, first, 0), (layers, own, width))
        own_core = lax.dynamic_slice(w_core, (0, first, 0, 0), (layers, own, rank, rank))
        grad_rows = lax.dynamic_slice(grad_out, (t * rows, 0), (rows, heads))
        grad_low = round_low(jnp.concatenate([grad_rows, swap(grad_rows)], axis=0))

        def matrices(full):
            full = full.reshape(tp, 2 * own, tiles, shard, 128)
            return pl.pallas_call(
                unpack_kernel,
                grid=(2 * own, tp),
                in_specs=[pl.BlockSpec((1, 1, tiles, shard, 128), lambda m, x: (x, m, 0, 0, 0))],
                out_specs=pl.BlockSpec((1, shard, rank), lambda m, x: (m, x, 0)),
                out_shape=jax.ShapeDtypeStruct((2 * own, width, rank), BF),
                cost_estimate=cost(20_000_000, 12 * own * width * rank),
            )(full)

        def outer(left, right):
            out = pl.pallas_call(
                outer_kernel,
                grid=(own, tp),
                in_specs=[pl.BlockSpec((shard, left.shape[1]), lambda e, x: (x, 0)),
                          pl.BlockSpec((1, rank, left.shape[1]), lambda e, x: (e, 0, 0))],
                out_specs=pl.BlockSpec((1, tiles, 2, 1, half, 128), lambda e, x: (e, 0, 0, x, 0, 0)),
                out_shape=jax.ShapeDtypeStruct((own, tiles, 2, tp, half, 128), F32),
                cost_estimate=cost(2 * own * rank * width * left.shape[1], 4 * own * rank * width),
            )(left, right)
            return out.reshape(plane, tp * half, 128)

        parts = []

        def scatter(blocks):
            if parts:
                blocks, parts[-1] = lax.optimization_barrier((blocks, parts[-1]))
            parts.append(lax.psum_scatter(blocks, PLANE, scatter_dimension=0, tiled=False))

        weights, saved = [], []
        state = feat.astype(BF)
        for layer in range(layers):
            full = gathered[layer]
            if layer:
                full, state = lax.optimization_barrier((full, state))
            w_all = matrices(full)
            down_w, up_t = w_all[:own], w_all[own:]
            weights.append((down_w, up_t))
            act_one = jnp.tanh(mm('ewr,wn->ern', down_w, state))
            gate = jax.nn.softmax(mm('ew,wn->en', gate_w[layer], state), axis=0)
            own_share = lax.dynamic_slice(gate, (first, 0), (own, gate.shape[1]))[:, None, :]
            act_low = act_one.astype(BF)
            act_two = jnp.tanh(mm('ers,ern->esn', own_core[layer], act_low))
            mixed = (own_share * act_two).astype(BF)
            mix_bias = both(mm('ewr,ern->wn', up_t, mixed)) + bias[layer][:, None]
            saved.append((state, act_one, act_low, act_two, own_share, mixed, mix_bias))
            state = (state.astype(F32) + feat * mix_bias).astype(BF)
        top_w = round_low(top_all[:, :top_len].reshape(width, heads))
        top_rows = mm('wn,wh->nh', state[:, :rows], top_w)
        top_out = jnp.zeros((tp, rows, heads), F32)
        top_out = lax.dynamic_update_slice(top_out, top_rows[None], (t, 0, 0))
        for shift in range(1, tp):
            part = lax.ppermute(top_rows, 'tp', [(i, (i + shift) % tp) for i in range(tp)])
            top_out = lax.dynamic_update_slice(top_out, part[None], ((t - shift) % tp, 0, 0))
        top_out = top_out.reshape(tp * rows, heads)

        grad_state = mm('wh,nh->wn', top_w, grad_low)
        own_state = lax.dynamic_slice(state.reshape(tp, shard, -1), (0, core * half, 0), (tp, half, state.shape[1]))
        grad_top = mm('xwn,nh->xwh', own_state, grad_low)
        grad_feat = jnp.zeros((width, rows), F32)
        core_grads, small_grads = [None] * layers, [None] * layers
        outs = None
        spec = pl.BlockSpec((1, tiles, 2, 2, half, 128), lambda e: (e % own, 0, 0, 0, 0, 0))
        core_id = core.astype(jnp.int32).reshape(1)
        for layer in reversed(range(layers)):
            state_in, act_one, act_low, act_two, own_share, mixed, mix_bias = saved[layer]
            down_w, up_t = weights[layer]
            grad_feat = grad_feat + grad_state[:, :rows] * mix_bias[:, :rows]
            grad_mix = grad_state * feat
            grad_bias = jnp.sum(grad_mix, axis=1)
            grad_mix_low = grad_mix.astype(BF)
            blocks, grad_mix_low = lax.optimization_barrier((outer(grad_mix_low, mixed), grad_mix_low))
            scatter(blocks)
            grad_mixed = mm('ewr,wn->ern', up_t, grad_mix_low)
            gate_act = jnp.sum(grad_mixed * act_two, axis=1)
            grad_mid = (grad_mixed * own_share * (1.0 - act_two * act_two)).astype(BF)
            core_grads[layer] = mm('ern,esn->ers', act_low, grad_mid)
            grad_act = mm('ers,esn->ern', own_core[layer], grad_mid)
            grad_proj = (grad_act * (1.0 - act_one * act_one)).astype(BF)
            blocks, grad_proj = lax.optimization_barrier((outer(state_in, grad_proj), grad_proj))
            scatter(blocks)
            share = own_share[:, 0]
            total = both(jnp.sum(share * gate_act, axis=0, keepdims=True))
            grad_logit = (share * (gate_act - total)).astype(BF)
            grad_gate = mm('en,wn->ew', grad_logit, state_in)
            small_grads[layer] = jnp.concatenate([grad_gate, grad_bias[None]], axis=0)
            part = mm('ewr,ern->wn', down_w, grad_proj) + mm('ew,en->wn', own_gate[layer], grad_logit)
            grad_state = grad_state + both(part)
        grad_feat = grad_feat + grad_state[:, :rows]
        grad_feat = lax.all_to_all(grad_feat.reshape(tp, shard, rows), 'tp', 0, 0)
        grad_feat = grad_feat.transpose(1, 0, 2).reshape(shard, tp * rows).T

        lanes = rank
        small_rows = layers * (own + 1)
        core_all = jnp.stack(core_grads).reshape(plane, tp, -1, lanes)
        core_len = core_all.shape[2]
        pad_rows = -half % (8 * plane)
        top_cut = jnp.pad(grad_top, ((0, 0), (0, pad_rows), (0, 0))).reshape(tp, plane, -1, lanes).transpose(1, 0, 2, 3)
        small_cut = jnp.stack(small_grads).reshape(small_rows, tp, shard).transpose(1, 0, 2)
        small_cut = jnp.pad(small_cut, ((0, 0), (0, plane - small_rows), (0, lanes - shard)))[:, :, None]
        small_cut = jnp.pad(small_cut.transpose(1, 0, 2, 3), ((0, 0), (0, 0), (0, 7), (0, 0)))
        misc = jnp.concatenate([core_all, top_cut, small_cut], axis=2)
        misc = misc.reshape(plane, -1, lanes)
        scatter(misc)
        for step, layer in enumerate(reversed(range(layers))):
            part = jnp.concatenate([parts[2 * step].reshape(tp, half, 128), parts[2 * step + 1].reshape(tp, half, 128)], axis=1)
            part = lax.psum_scatter(part.reshape(tp * shard, 128), 'tp', scatter_dimension=0, tiled=True)
            mine = lax.all_gather(part, PLANE, axis=0)
            theirs = swap(mine)
            operands = [v.reshape(own, tiles, 2, 2, half, 128) for v in (mine, theirs)]
            place = pl.BlockSpec((1, 1, shard, rank), lambda e, layer=layer: (layer, e, 0, 0))
            outs = pl.pallas_call(
                place_kernel,
                grid=(experts,),
                in_specs=[pl.BlockSpec(memory_space=pltpu.SMEM), spec, spec] + [pl.BlockSpec(memory_space=pl.ANY)] * (2 if outs else 0),
                out_specs=[place, place],
                out_shape=[jax.ShapeDtypeStruct((layers, experts, shard, rank), F32)] * 2,
                input_output_aliases={3: 0, 4: 1} if outs else {},
                cost_estimate=cost(8_000_000, 24 * experts * shard * rank),
            )(core_id, *operands, *(outs or ()))
        part = lax.psum_scatter(parts[-1], 'tp', scatter_dimension=0, tiled=True)
        cores = lax.all_gather(part[:core_len], CHIPS, axis=0)
        cores = cores.reshape(tp, plane, core_len, lanes).transpose(1, 0, 2, 3).reshape(layers, own, rank, rank)
        rest = lax.all_gather(part[core_len:], PLANE, axis=0)

        def paired(values, axis):
            other = swap(values)
            return jnp.where(core == 0, jnp.concatenate([values, other], axis=axis), jnp.concatenate([other, values], axis=axis))

        core_out = paired(cores, 1)
        rest = paired(rest[None], 0)
        top_res = rest[:, :, :-8].reshape(2, half + pad_rows, heads)[:, :half].reshape(shard, heads)
        small_res = rest[:, :small_rows, -8, :shard].reshape(2, layers, own + 1, shard)
        gate_out = small_res[:, :, :own].transpose(1, 3, 0, 2).reshape(layers, shard, experts)
        bias_out = small_res[0, :, own]
        return top_out, grad_feat, outs[0], core_out, outs[1].transpose(0, 1, 3, 2), gate_out, bias_out, top_res

    dp = ('z', 'y', 'core')
    in_specs = (P(dp, 'tp'), P(dp, None), P(None, None, 'tp', None), P(), P(None, None, None, 'tp'), P(None, 'tp', None), P(None, 'tp'), P('tp', None))
    out_specs = (P(dp, None), P(dp, 'tp'), P(None, None, 'tp', None), P(), P(None, None, None, 'tp'), P(None, 'tp', None), P(None, 'tp'), P('tp', None))
    return jax.shard_map(device_body, mesh=mesh, in_specs=in_specs, out_specs=out_specs, check_vma=False)
```

```python
import jax
import jax.numpy as jnp
from jax import lax
from jax.experimental import pallas as pl
from jax.experimental.pallas import tpu as pltpu
from jax.sharding import Mesh, PartitionSpec as P

BF = jnp.bfloat16
F32 = jnp.float32
PLANE = ('z', 'y', 'core')


def cost(flops, nbytes):
    return pl.CostEstimate(flops=flops, bytes_accessed=nbytes, transcendentals=0)


def unpack_kernel(where_ref, local_ref, *refs):
    pieces, out_ref = refs[:-1], refs[-1]
    far = len(pieces) // 3
    for i in range(far):
        for j in range(4):
            @pl.when((pl.program_id(0) == i) & (pl.program_id(1) == j))
            def _():
                if j == 0:
                    out_ref[0] = local_ref[0]
                else:
                    out_ref[0] = pieces[i * 3 + j - 1][...].astype(BF)


def round_kernel(in_ref, out_ref):
    out_ref[...] = in_ref[...].astype(BF)


def round_low(values):
    return pl.pallas_call(round_kernel, out_shape=jax.ShapeDtypeStruct(values.shape, BF))(values)


def outer_kernel(left_ref, right_ref, out_ref):
    prod = lax.dot_general(left_ref[...], right_ref[0], (((1,), (1,)), ((), ())), preferred_element_type=F32)
    half = out_ref.shape[3]
    for h in range(2):
        out_ref[0, h, 0] = prod[h * half:(h + 1) * half]


def place_kernel(core_ref, mine_down, theirs_down, mine_up, theirs_up, *refs):
    down_ref, up_ref = refs[-2:]
    own = (pl.program_id(0) // 2 == core_ref[0])
    down_ref[0, 0] = jnp.where(own, mine_down[0], theirs_down[0])
    up_ref[0, 0] = jnp.where(own, mine_up[0], theirs_up[0])


def solution(mesh):
    tp = mesh.shape['tp']
    mesh = Mesh(mesh.devices.reshape(tp, 4, 4, 2), ('tp', 'z', 'y', 'core'))

    def ring(axis, step):
        pairs = []
        for z in range(4):
            for y in range(4):
                for c in range(2):
                    along_y = (axis == 'a') == (c == 0)
                    to_z, to_y = (z, (y + step) % 4) if along_y else ((z + step) % 4, y)
                    pairs.append((z * 8 + y * 2 + c, to_z * 8 + to_y * 2 + c))
        return pairs

    def hop(values, axis, step):
        if axis == 'x':
            return lax.ppermute(values, 'tp', [(i, (i + step) % 4) for i in range(4)])
        return lax.ppermute(values, PLANE, ring(axis, step))

    def finite(values):
        return jnp.clip(values, jnp.finfo(F32).min, jnp.finfo(F32).max)

    def mm(spec, a, b):
        return jnp.einsum(spec, a, b, preferred_element_type=F32)

    def swap(values):
        return lax.ppermute(values, 'core', [(0, 1), (1, 0)])

    def flip(values):
        half = values.shape[-1] // 2
        return jnp.concatenate([values[..., half:], values[..., :half]], axis=-1)

    def both(part):
        return part + flip(swap(part))

    def device_body(feat_in, grad_out, w_down, w_core, w_up, w_gate, bias_cross, w_top):
        layers, experts, shard, rank = w_down.shape
        rows = feat_in.shape[0] // tp
        width = shard * tp
        heads = w_top.shape[1]
        own = experts // 2
        t = lax.axis_index('tp')
        core = lax.axis_index('core')
        z, y = lax.axis_index('z'), lax.axis_index('y')
        spot = {'x': t, 'a': jnp.where(core == 0, y, z), 'b': jnp.where(core == 0, z, y)}
        half = shard // 2
        first = core * own

        def gather(values, axis):
            cut = values.shape[0] // 2
            back, ahead = hop(values, axis, 1), hop(values, axis, -1)
            far = jnp.concatenate([hop(back[:cut], axis, 1), hop(ahead[cut:], axis, -1)], axis=0)
            return [values, ahead, far, back]

        def gather_way(values, axis, step):
            near, other = hop(values, axis, step), hop(values, axis, -step)
            far = hop(near, axis, step)
            return [values, other, far, near] if step == 1 else [values, near, far, other]

        def reduce_way(values, dim, axis, step):
            def part(away):
                return lax.dynamic_index_in_dim(values, (spot[axis] + away) % 4, dim, keepdims=False)

            relay = hop(part(2 * step), axis, step)
            near = hop(part(-step), axis, -step)
            return part(0) + near + hop(part(step) + relay, axis, step)

        def ordered(pieces, axis, dim):
            shape = list(pieces[0].shape)
            size = shape[dim]
            shape[dim] = 4 * size
            out = jnp.zeros(shape, F32)
            for away, piece in enumerate(pieces):
                out = lax.dynamic_update_slice_in_dim(out, piece, ((spot[axis] + away) % 4) * size, dim)
            return out

        up_turned = w_up.transpose(0, 1, 3, 2)
        local = jnp.concatenate([lax.dynamic_slice(w_down, (0, first, 0, 0), (layers, own, shard, rank)),
                                 lax.dynamic_slice(up_turned, (0, first, 0, 0), (layers, own, shard, rank))], axis=1)
        pieces = lax.dynamic_index_in_dim(local, spot['a'], 1, keepdims=False)
        pieces = finite(pieces.astype(F32))
        gathered = []
        for layer in range(layers):
            across = gather(pieces[layer], 'x')[1:]
            blocks = [gather(block, 'a') for block in across]
            gathered.append([blocks[j][i] for i in range(4) for j in range(3)])
        top_pieces = gather(finite(w_top.astype(F32)), 'x')[1:]
        where = jnp.stack([spot['a'], t]).astype(jnp.int32)

        send = finite(feat_in.T.astype(F32)).reshape(shard, tp, rows).transpose(1, 0, 2)
        got = lax.all_to_all(send, 'tp', 0, 0).reshape(width, rows)
        feat = jnp.concatenate([got, swap(got)], axis=1)
        small = jnp.concatenate([w_gate.transpose(0, 2, 1), bias_cross[:, None, :]], axis=1)
        small = finite(small.reshape(layers * (experts + 1), shard).astype(F32))
        small = lax.all_gather(small, 'tp', axis=0).transpose(1, 0, 2).reshape(layers, experts + 1, width)
        gate_w = small[:, :experts].astype(BF)
        bias = small[:, experts]
        own_gate = lax.dynamic_slice(gate_w, (0, first, 0), (layers, own, width))
        own_core = lax.dynamic_slice(w_core, (0, first, 0, 0), (layers, own, rank, rank))
        grad_rows = lax.dynamic_slice(grad_out, (t * rows, 0), (rows, heads))
        grad_low = round_low(jnp.concatenate([grad_rows, swap(grad_rows)], axis=0))

        def matrices(local_part, parts):
            mats = local_part.shape[0]
            return pl.pallas_call(
                unpack_kernel,
                grid_spec=pltpu.PrefetchScalarGridSpec(
                    num_scalar_prefetch=1,
                    grid=(mats, tp),
                    in_specs=[pl.BlockSpec((1, shard, rank), lambda i, j, at: ((at[0] + i) % mats, 0, 0))]
                    + [pl.BlockSpec((shard, rank), lambda i, j, at: (0, 0))] * len(parts),
                    out_specs=pl.BlockSpec((1, shard, rank), lambda i, j, at: ((at[0] + i) % mats, (at[1] + j) % 4, 0)),
                ),
                out_shape=jax.ShapeDtypeStruct((mats, width, rank), BF),
                cost_estimate=cost(20_000_000, 6 * mats * width * rank),
            )(where, local_part, *parts)

        def outer(left, right):
            out = pl.pallas_call(
                outer_kernel,
                grid=(own, tp),
                in_specs=[pl.BlockSpec((shard, left.shape[1]), lambda e, x: (x, 0)),
                          pl.BlockSpec((1, rank, left.shape[1]), lambda e, x: (e, 0, 0))],
                out_specs=pl.BlockSpec((1, 2, 1, half, rank), lambda e, x: (e, 0, x, 0, 0)),
                out_shape=jax.ShapeDtypeStruct((own, 2, tp, half, rank), F32),
                cost_estimate=cost(2 * own * rank * width * left.shape[1], 4 * own * rank * width),
            )(left, right)
            return out.reshape(2 * own, tp, half, rank)

        weights, saved = [], []
        state = feat.astype(BF)
        for layer in range(layers):
            parts = gathered[layer]
            early = [(layer + 1, k) for k in (0, 1, 2, 3, 4, 5, 9, 10, 11)] + [(layer + 2, k) for k in (0, 1, 2)]
            early = [(n, k) for n, k in early if n < layers]
            parts, state, tied = lax.optimization_barrier((parts, state, [gathered[n][k] for n, k in early]))
            for (n, k), value in zip(early, tied):
                gathered[n][k] = value
            w_all = matrices(local[layer], parts)
            down_w, up_t = w_all[:own], w_all[own:]
            weights.append((down_w, up_t))
            act_one = jnp.tanh(mm('ewr,wn->ern', down_w, state))
            gate = jax.nn.softmax(mm('ew,wn->en', gate_w[layer], state), axis=0)
            own_share = lax.dynamic_slice(gate, (first, 0), (own, gate.shape[1]))[:, None, :]
            act_low = act_one.astype(BF)
            act_two = jnp.tanh(mm('ers,ern->esn', own_core[layer], act_low))
            mixed = (own_share * act_two).astype(BF)
            mix_bias = both(mm('ewr,ern->wn', up_t, mixed)) + bias[layer][:, None]
            saved.append((state, act_one, act_low, act_two, own_share, mixed, mix_bias))
            state = (state.astype(F32) + feat * mix_bias).astype(BF)
        top_w = matrices(w_top[None], top_pieces)[0]
        top_rows = mm('wn,wh->nh', state[:, :rows], top_w)
        top_out = jnp.zeros((tp, rows, heads), F32)
        top_out = lax.dynamic_update_slice(top_out, top_rows[None], (t, 0, 0))
        for shift in range(1, tp):
            part = lax.ppermute(top_rows, 'tp', [(i, (i + shift) % tp) for i in range(tp)])
            top_out = lax.dynamic_update_slice(top_out, part[None], ((t - shift) % tp, 0, 0))
        top_out = top_out.reshape(tp * rows, heads)

        grad_state = mm('wh,nh->wn', top_w, grad_low)
        own_state = lax.dynamic_slice(state.reshape(tp, shard, -1), (0, core * half, 0), (tp, half, state.shape[1]))
        grad_top = mm('xwn,nh->xwh', own_state, grad_low)
        grad_feat = jnp.zeros((width, rows), F32)
        reduced = [None] * layers

        def reduce_pair(up_blocks, down_blocks, across_first):
            outs = []
            for blocks, step in ((up_blocks, 1), (down_blocks, -1)):
                if across_first:
                    part = reduce_way(reduce_way(blocks, 1, 'x', step), 0, 'a', step)
                else:
                    part = reduce_way(reduce_way(blocks, 0, 'a', step), 0, 'x', step)
                part = reduce_way(part.reshape(half, 4, rank // 4), 1, 'b', step)
                part = ordered(gather_way(part, 'b', step), 'b', 1)
                outs.append(ordered(gather_way(part[None], 'a', step), 'a', 0).reshape(own, shard, rank))
            return outs

        core_grads, small_grads = [None] * layers, [None] * layers
        outs = None
        spec = pl.BlockSpec((1, shard, rank), lambda e: (e % own, 0, 0))
        core_id = core.astype(jnp.int32).reshape(1)
        for layer in reversed(range(layers)):
            state_in, act_one, act_low, act_two, own_share, mixed, mix_bias = saved[layer]
            down_w, up_t = weights[layer]
            grad_feat = grad_feat + grad_state[:, :rows] * mix_bias[:, :rows]
            grad_mix = grad_state * feat
            grad_bias = jnp.sum(grad_mix, axis=1)
            grad_mix_low = grad_mix.astype(BF)
            blocks, grad_mix_low = lax.optimization_barrier((outer(grad_mix_low, mixed), grad_mix_low))
            up_blocks = blocks
            grad_mixed = mm('ewr,wn->ern', up_t, grad_mix_low)
            gate_act = jnp.sum(grad_mixed * act_two, axis=1)
            grad_mid = (grad_mixed * own_share * (1.0 - act_two * act_two)).astype(BF)
            core_grads[layer] = mm('ern,esn->ers', act_low, grad_mid)
            grad_act = mm('ers,esn->ern', own_core[layer], grad_mid)
            grad_proj = (grad_act * (1.0 - act_one * act_one)).astype(BF)
            blocks, grad_proj = lax.optimization_barrier((outer(state_in, grad_proj), grad_proj))
            reduced[layer] = reduce_pair(up_blocks, blocks, layer == layers - 1)
            share = own_share[:, 0]
            total = both(jnp.sum(share * gate_act, axis=0, keepdims=True))
            grad_logit = (share * (gate_act - total)).astype(BF)
            grad_gate = mm('en,wn->ew', grad_logit, state_in)
            small_grads[layer] = jnp.concatenate([grad_gate, grad_bias[None]], axis=0)
            part = mm('ewr,ern->wn', down_w, grad_proj) + mm('ew,en->wn', own_gate[layer], grad_logit)
            grad_state = grad_state + both(part)
        grad_feat = grad_feat + grad_state[:, :rows]
        grad_feat = lax.all_to_all(grad_feat.reshape(tp, shard, rows), 'tp', 0, 0)
        grad_feat = grad_feat.transpose(1, 0, 2).reshape(shard, tp * rows).T

        for layer in reversed(range(layers)):
            up_mine, down_mine = reduced[layer]
            operands = [down_mine, swap(down_mine), up_mine, swap(up_mine)]
            place = pl.BlockSpec((1, 1, shard, rank), lambda e, layer=layer: (layer, e, 0, 0))
            outs = pl.pallas_call(
                place_kernel,
                grid=(experts,),
                in_specs=[pl.BlockSpec(memory_space=pltpu.SMEM)] + [spec] * 4 + [pl.BlockSpec(memory_space=pl.ANY)] * (2 if outs else 0),
                out_specs=[place, place],
                out_shape=[jax.ShapeDtypeStruct((layers, experts, shard, rank), F32)] * 2,
                input_output_aliases={5: 0, 6: 1} if outs else {},
                cost_estimate=cost(8_000_000, 24 * experts * shard * rank),
            )(core_id, *operands, *(outs or ()))

        lanes = rank
        small_rows = layers * (own + 1)
        core_part = jnp.stack(core_grads).reshape(4, tp, 4, -1, lanes)
        for dim, axis in ((0, 'a'), (0, 'x'), (0, 'b')):
            core_part = reduce_way(core_part, dim, axis, 1)
        for axis in ('b', 'x', 'a'):
            core_part = ordered(gather_way(core_part, axis, 1), axis, 0)
        cores = core_part.reshape(layers, own, rank, rank)
        pad_rows = -half % 128
        top_cut = jnp.pad(grad_top, ((0, 0), (0, pad_rows), (0, 0))).reshape(tp, 4, 4, -1, lanes).transpose(1, 0, 2, 3, 4)
        small_cut = jnp.stack(small_grads).reshape(small_rows, tp, shard).transpose(1, 0, 2)
        small_cut = jnp.pad(small_cut, ((0, 0), (0, 16 - small_rows), (0, lanes - shard)))
        small_cut = small_cut.reshape(tp, 4, 4, 1, lanes).transpose(1, 0, 2, 3, 4)
        small_cut = jnp.pad(small_cut, ((0, 0), (0, 0), (0, 0), (0, 7), (0, 0)))
        rest = jnp.concatenate([top_cut, small_cut], axis=3)
        for axis in ('a', 'x', 'b'):
            rest = reduce_way(rest, 0, axis, -1)
        for axis in ('b', 'a'):
            rest = ordered(gather_way(rest[None], axis, -1), axis, 0)
        rest = rest.reshape((16,) + rest.shape[-2:])

        def paired(values, axis):
            other = swap(values)
            return jnp.where(core == 0, jnp.concatenate([values, other], axis=axis), jnp.concatenate([other, values], axis=axis))

        core_out = paired(cores, 1)
        rest = paired(rest[None], 0)
        top_res = rest[:, :, :-8].reshape(2, half + pad_rows, heads)[:, :half].reshape(shard, heads)
        small_res = rest[:, :small_rows, -8, :shard].reshape(2, layers, own + 1, shard)
        gate_out = small_res[:, :, :own].transpose(1, 3, 0, 2).reshape(layers, shard, experts)
        bias_out = small_res[0, :, own]
        return top_out, grad_feat, outs[0], core_out, outs[1].transpose(0, 1, 3, 2), gate_out, bias_out, top_res

    dp = ('z', 'y', 'core')
    in_specs = (P(dp, 'tp'), P(dp, None), P(None, None, 'tp', None), P(), P(None, None, None, 'tp'), P(None, 'tp', None), P(None, 'tp'), P('tp', None))
    out_specs = (P(dp, None), P(dp, 'tp'), P(None, None, 'tp', None), P(), P(None, None, None, 'tp'), P(None, 'tp', None), P(None, 'tp'), P('tp', None))
    return jax.shard_map(device_body, mesh=mesh, in_specs=in_specs, out_specs=out_specs, check_vma=False)
```

```python
import jax
import jax.numpy as jnp
from jax import lax
from jax.experimental import pallas as pl
from jax.experimental.pallas import tpu as pltpu
from jax.sharding import Mesh, PartitionSpec as P

BF = jnp.bfloat16
F32 = jnp.float32
PLANE = ('z', 'y', 'core')


def cost(flops, nbytes):
    return pl.CostEstimate(flops=flops, bytes_accessed=nbytes, transcendentals=0)


def unpack_kernel(where_ref, local_ref, *refs):
    pieces, out_ref = refs[:-1], refs[-1]
    for i in range(len(pieces)):
        for j in range(4):
            @pl.when((pl.program_id(0) == i) & (pl.program_id(1) == j))
            def _():
                if j == 0:
                    out_ref[0] = local_ref[0]
                else:
                    out_ref[0] = pieces[i][j - 1].astype(BF)


def round_kernel(in_ref, out_ref):
    out_ref[...] = in_ref[...].astype(BF)


def round_low(values):
    return pl.pallas_call(round_kernel, out_shape=jax.ShapeDtypeStruct(values.shape, BF))(values)


def outer_kernel(left_ref, right_ref, out_ref):
    prod = lax.dot_general(left_ref[...], right_ref[0], (((1,), (1,)), ((), ())), preferred_element_type=F32)
    half = out_ref.shape[3]
    for h in range(2):
        out_ref[0, h, 0] = prod[h * half:(h + 1) * half]


def place_kernel(core_ref, mine_up, theirs_up, mine_down, theirs_down, *refs):
    down_ref, up_ref = refs[-2:]
    own = (pl.program_id(0) // 2 == core_ref[0])
    half = mine_up.shape[1]
    for h in range(2):
        down_ref[0, 0, h * half:(h + 1) * half] = jnp.where(own, mine_down[h], theirs_down[h])
        up_ref[0, 0, h * half:(h + 1) * half] = jnp.where(own, mine_up[h], theirs_up[h])


def solution(mesh):
    tp = mesh.shape['tp']
    mesh = Mesh(mesh.devices.reshape(tp, 4, 4, 2), ('tp', 'z', 'y', 'core'))

    def ring(axis, step):
        pairs = []
        for z in range(4):
            for y in range(4):
                for c in range(2):
                    along_y = (axis == 'a') == (c == 0)
                    to_z, to_y = (z, (y + step) % 4) if along_y else ((z + step) % 4, y)
                    pairs.append((z * 8 + y * 2 + c, to_z * 8 + to_y * 2 + c))
        return pairs

    def hop(values, axis, step):
        if axis == 'x':
            return lax.ppermute(values, 'tp', [(i, (i + step) % 4) for i in range(4)])
        return lax.ppermute(values, PLANE, ring(axis, step))

    def finite(values):
        return jnp.clip(values, jnp.finfo(F32).min, jnp.finfo(F32).max)

    def mm(spec, a, b):
        return jnp.einsum(spec, a, b, preferred_element_type=F32)

    def swap(values):
        return lax.ppermute(values, 'core', [(0, 1), (1, 0)])

    def flip(values):
        half = values.shape[-1] // 2
        return jnp.concatenate([values[..., half:], values[..., :half]], axis=-1)

    def both(part):
        return part + flip(swap(part))

    def device_body(feat_in, grad_out, w_down, w_core, w_up, w_gate, bias_cross, w_top):
        layers, experts, shard, rank = w_down.shape
        rows = feat_in.shape[0] // tp
        width = shard * tp
        heads = w_top.shape[1]
        own = experts // 2
        t = lax.axis_index('tp')
        core = lax.axis_index('core')
        z, y = lax.axis_index('z'), lax.axis_index('y')
        spot = {'x': t, 'a': jnp.where(core == 0, y, z), 'b': jnp.where(core == 0, z, y)}
        half = shard // 2
        first = core * own

        def gather(values, axis):
            cut = values.shape[-2] // 2
            back, ahead = hop(values, axis, 1), hop(values, axis, -1)
            far = jnp.concatenate([hop(back[..., :cut, :], axis, 1), hop(ahead[..., cut:, :], axis, -1)], axis=-2)
            return [values, ahead, far, back]

        def gather_way(values, axis, step):
            near, other = hop(values, axis, step), hop(values, axis, -step)
            far = hop(near, axis, step)
            return [values, other, far, near] if step == 1 else [values, near, far, other]

        def reduce_way(values, dim, axis, step):
            size = values.shape[dim] // 4

            def part(away):
                piece = lax.dynamic_slice_in_dim(values, (spot[axis] + away) % 4 * size, size, dim)
                return jnp.squeeze(piece, dim) if size == 1 else piece

            relay = hop(part(2 * step), axis, step)
            near = hop(part(-step), axis, -step)
            return part(0) + near + hop(part(step) + relay, axis, step)

        def ordered(pieces, axis, dim):
            shape = list(pieces[0].shape)
            size = shape[dim]
            shape[dim] = 4 * size
            out = jnp.zeros(shape, F32)
            for away, piece in enumerate(pieces):
                out = lax.dynamic_update_slice_in_dim(out, piece, ((spot[axis] + away) % 4) * size, dim)
            return out

        up_turned = w_up.transpose(0, 1, 3, 2)
        local = jnp.concatenate([lax.dynamic_slice(w_down, (0, first, 0, 0), (layers, own, shard, rank)),
                                 lax.dynamic_slice(up_turned, (0, first, 0, 0), (layers, own, shard, rank))], axis=1)
        pieces = lax.dynamic_index_in_dim(local, spot['a'], 1, keepdims=False)
        pieces = finite(pieces.astype(F32))
        small = jnp.concatenate([w_gate.transpose(0, 2, 1), bias_cross[:, None, :]], axis=1)
        small_count = layers * (experts + 1)
        small = finite(small.reshape(small_count, shard).astype(F32))
        small = jnp.pad(small, ((0, -small_count % 16), (0, rank - shard)))
        head = gather(jnp.concatenate([pieces[0], small], axis=0), 'x')
        small = ordered([part[None, shard:] for part in head], 'x', 0)
        small = small[:, :small_count, :shard].transpose(1, 0, 2).reshape(layers, experts + 1, width)
        others = gather(jnp.concatenate([pieces[1:], finite(w_top.astype(F32))[None]], axis=0), 'x')[1:]
        stacks = [jnp.stack([part[:shard] for part in head[1:]])]
        stacks += [jnp.stack([part[n] for part in others]) for n in range(layers)]
        gathered = [gather(stack, 'a') for stack in stacks[:layers]]
        top_pieces = [stacks[layers]]
        where = jnp.stack([spot['a'], t]).astype(jnp.int32)

        send = finite(feat_in.T.astype(F32)).reshape(shard, tp, rows).transpose(1, 0, 2)
        got = lax.all_to_all(send, 'tp', 0, 0).reshape(width, rows)
        feat = jnp.concatenate([got, swap(got)], axis=1)
        gate_w = small[:, :experts].astype(BF)
        bias = small[:, experts]
        own_gate = lax.dynamic_slice(gate_w, (0, first, 0), (layers, own, width))
        own_core = lax.dynamic_slice(w_core, (0, first, 0, 0), (layers, own, rank, rank))
        grad_rows = lax.dynamic_slice(grad_out, (t * rows, 0), (rows, heads))
        grad_low = round_low(jnp.concatenate([grad_rows, swap(grad_rows)], axis=0))

        def matrices(local_part, parts):
            mats = local_part.shape[0]
            return pl.pallas_call(
                unpack_kernel,
                grid_spec=pltpu.PrefetchScalarGridSpec(
                    num_scalar_prefetch=1,
                    grid=(mats, tp),
                    in_specs=[pl.BlockSpec((1, shard, rank), lambda i, j, at: ((at[0] + i) % mats, 0, 0))]
                    + [pl.BlockSpec((3, shard, rank), lambda i, j, at: (0, 0, 0))] * len(parts),
                    out_specs=pl.BlockSpec((1, shard, rank), lambda i, j, at: ((at[0] + i) % mats, (at[1] + j) % 4, 0)),
                ),
                out_shape=jax.ShapeDtypeStruct((mats, width, rank), BF),
                cost_estimate=cost(20_000_000, 6 * mats * width * rank),
            )(where, local_part, *parts)

        def outer(left, right):
            out = pl.pallas_call(
                outer_kernel,
                grid=(own, tp),
                in_specs=[pl.BlockSpec((shard, left.shape[1]), lambda e, x: (x, 0)),
                          pl.BlockSpec((1, rank, left.shape[1]), lambda e, x: (e, 0, 0))],
                out_specs=pl.BlockSpec((1, 2, 1, half, rank), lambda e, x: (e, 0, x, 0, 0)),
                out_shape=jax.ShapeDtypeStruct((own, 2, tp, half, rank), F32),
                cost_estimate=cost(2 * own * rank * width * left.shape[1], 4 * own * rank * width),
            )(left, right)
            return out.reshape(2 * own, tp, half, rank)

        weights, saved = [], []
        state = feat.astype(BF)
        for layer in range(layers):
            parts = gathered[layer]
            early = [(layer + 1, k) for k in (0, 1, 3)] + [(layer + 2, 0)]
            early = [(n, k) for n, k in early if n < layers]
            parts, state, tied = lax.optimization_barrier((parts, state, [gathered[n][k] for n, k in early]))
            for (n, k), value in zip(early, tied):
                gathered[n][k] = value
            w_all = matrices(local[layer], parts)
            down_w, up_t = w_all[:own], w_all[own:]
            weights.append((down_w, up_t))
            act_one = jnp.tanh(mm('ewr,wn->ern', down_w, state))
            gate = jax.nn.softmax(mm('ew,wn->en', gate_w[layer], state), axis=0)
            own_share = lax.dynamic_slice(gate, (first, 0), (own, gate.shape[1]))[:, None, :]
            act_low = act_one.astype(BF)
            act_two = jnp.tanh(mm('ers,ern->esn', own_core[layer], act_low))
            mixed = (own_share * act_two).astype(BF)
            mix_bias = both(mm('ewr,ern->wn', up_t, mixed)) + bias[layer][:, None]
            saved.append((state, act_one, act_low, act_two, own_share, mixed, mix_bias))
            state = (state.astype(F32) + feat * mix_bias).astype(BF)
        top_w = matrices(w_top[None], top_pieces)[0]
        top_rows = mm('wn,wh->nh', state[:, :rows], top_w)
        top_out = jnp.zeros((tp, rows, heads), F32)
        top_out = lax.dynamic_update_slice(top_out, top_rows[None], (t, 0, 0))
        for shift in range(1, tp):
            part = lax.ppermute(top_rows, 'tp', [(i, (i + shift) % tp) for i in range(tp)])
            top_out = lax.dynamic_update_slice(top_out, part[None], ((t - shift) % tp, 0, 0))
        top_out = top_out.reshape(tp * rows, heads)

        grad_state = mm('wh,nh->wn', top_w, grad_low)
        own_state = lax.dynamic_slice(state.reshape(tp, shard, -1), (0, core * half, 0), (tp, half, state.shape[1]))
        grad_top = mm('xwn,nh->xwh', own_state, grad_low)
        grad_feat = jnp.zeros((width, rows), F32)
        reduced = [None] * layers

        def reduce_pair(up_blocks, down_blocks, layer):
            if layer == layers - 1:
                pair = [reduce_way(up_blocks, 1, 'x', 1), reduce_way(down_blocks, 1, 'x', -1)]
            else:
                pair = [reduce_way(up_blocks, 0, 'a', 1), reduce_way(down_blocks, 0, 'a', -1)]
            if layer == 0:
                return pair
            pair = jnp.concatenate(pair, axis=1)
            return reduce_way(pair, 0, 'a' if layer == layers - 1 else 'x', 1 if layer % 2 else -1)

        def all_b(part, step):
            part = reduce_way(part, 1, 'b', step)
            return ordered(gather_way(part, 'b', step), 'b', 1)

        def all_a(part):
            return ordered([piece[None] for piece in gather(part, 'a')], 'a', 0)

        core_grads, small_grads = [None] * layers, [None] * layers
        outs = None
        core_id = core.astype(jnp.int32).reshape(1)
        for layer in reversed(range(layers)):
            state_in, act_one, act_low, act_two, own_share, mixed, mix_bias = saved[layer]
            if layer == layers - 2:
                grad_state, top_out = lax.optimization_barrier((grad_state, top_out))
            down_w, up_t = weights[layer]
            grad_feat = grad_feat + grad_state[:, :rows] * mix_bias[:, :rows]
            grad_mix = grad_state * feat
            grad_bias = jnp.sum(grad_mix, axis=1)
            grad_mix_low = grad_mix.astype(BF)
            blocks, grad_mix_low = lax.optimization_barrier((outer(grad_mix_low, mixed), grad_mix_low))
            up_blocks = blocks
            grad_mixed = mm('ewr,wn->ern', up_t, grad_mix_low)
            gate_act = jnp.sum(grad_mixed * act_two, axis=1)
            grad_mid = (grad_mixed * own_share * (1.0 - act_two * act_two)).astype(BF)
            core_grads[layer] = mm('ern,esn->ers', act_low, grad_mid)
            grad_act = mm('ers,esn->ern', own_core[layer], grad_mid)
            grad_proj = (grad_act * (1.0 - act_one * act_one)).astype(BF)
            blocks, grad_proj = lax.optimization_barrier((outer(state_in, grad_proj), grad_proj))
            reduced[layer] = reduce_pair(up_blocks, blocks, layer)
            share = own_share[:, 0]
            total = both(jnp.sum(share * gate_act, axis=0, keepdims=True))
            grad_logit = (share * (gate_act - total)).astype(BF)
            grad_gate = mm('en,wn->ew', grad_logit, state_in)
            small_grads[layer] = jnp.concatenate([grad_gate, grad_bias[None]], axis=0)
            part = mm('ewr,ern->wn', down_w, grad_proj) + mm('ew,en->wn', own_gate[layer], grad_logit)
            grad_state = grad_state + both(part)
        grad_feat = grad_feat + grad_state[:, :rows]
        grad_feat = lax.all_to_all(grad_feat.reshape(tp, shard, rows), 'tp', 0, 0)
        grad_feat = grad_feat.transpose(1, 0, 2).reshape(shard, tp * rows).T

        def place(outs, mine, theirs, layer, up_slot):
            spots = [pl.BlockSpec((2, half, rank), lambda e, n=n: (e % own, n, 0)) for n in (up_slot, up_slot, up_slot + 1, up_slot + 1)]
            target = pl.BlockSpec((1, 1, shard, rank), lambda e: (layer, e, 0, 0))
            return pl.pallas_call(
                place_kernel,
                grid=(experts,),
                in_specs=[pl.BlockSpec(memory_space=pltpu.SMEM)] + spots + [pl.BlockSpec(memory_space=pl.ANY)] * (2 if outs else 0),
                out_specs=[target, target],
                out_shape=[jax.ShapeDtypeStruct((layers, experts, shard, rank), F32)] * 2,
                input_output_aliases={5: 0, 6: 1} if outs else {},
                cost_estimate=cost(8_000_000, 24 * experts * shard * rank),
            )(core_id, mine, theirs, mine, theirs, *(outs or ()))

        upper = list(reversed(range(1, layers)))
        mine = all_a(all_b(jnp.concatenate([reduced[layer] for layer in upper], axis=0), -1))
        theirs = swap(mine)
        for n, layer in enumerate(upper):
            outs = place(outs, mine, theirs, layer, 2 * n)

        lanes = rank
        small_rows = layers * (own + 1)
        core_all = jnp.stack(core_grads).reshape(4, tp, -1, lanes)
        core_len = core_all.shape[2]
        pad_rows = -half % 32
        top_cut = jnp.pad(grad_top, ((0, 0), (0, pad_rows), (0, 0))).reshape(tp, 4, -1, lanes).transpose(1, 0, 2, 3)
        top_len = top_cut.shape[2]
        small_cut = jnp.stack(small_grads).reshape(small_rows, tp, shard).transpose(1, 0, 2)
        small_cut = jnp.pad(small_cut, ((0, 0), (0, 16 - small_rows), (0, lanes - shard)))
        small_cut = small_cut.reshape(tp, 4, 4, lanes).transpose(1, 0, 2, 3)
        small_cut = jnp.pad(small_cut, ((0, 0), (0, 0), (0, -(core_len + top_len + 4) % 16), (0, 0)))
        misc = reduce_way(jnp.concatenate([core_all, top_cut, small_cut], axis=2), 0, 'a', 1)
        total_len = misc.shape[1]
        cut = total_len // 2
        up_half, down_half = reduced[0]
        low = reduce_way(jnp.concatenate([up_half, misc[:, :cut]], axis=1), 0, 'x', 1)
        high = reduce_way(jnp.concatenate([down_half, misc[:, cut:]], axis=1), 0, 'x', -1)
        last = all_b(jnp.concatenate([low[:half], high[:half], low[half:], high[half:]], axis=0), 1)
        outs, grad_feat, last = lax.optimization_barrier((outs, grad_feat, last))
        cores = ordered(gather_way(last[shard:shard + core_len], 'x', 1), 'x', 0)
        mine = all_a(jnp.concatenate([last[:shard], cores, last[shard + core_len:]], axis=0))
        theirs = swap(mine)
        outs = place(outs, mine, theirs, 0, 0)

        def paired(values, other, axis):
            return jnp.where(core == 0, jnp.concatenate([values, other], axis=axis), jnp.concatenate([other, values], axis=axis))

        both_cores = [values[:, shard:shard + tp * core_len].reshape(layers, own, rank, rank) for values in (mine, theirs)]
        core_out = paired(*both_cores, 1)
        rest = paired(*[values[None, :, shard + tp * core_len:] for values in (mine, theirs)], 0)
        top_res = rest[:, :, :top_len].reshape(2, half + pad_rows, heads)[:, :half].reshape(shard, heads)
        small_res = rest[:, :, top_len:top_len + 4, :shard].reshape(2, 16, shard)[:, :small_rows].reshape(2, layers, own + 1, shard)
        gate_out = small_res[:, :, :own].transpose(1, 3, 0, 2).reshape(layers, shard, experts)
        bias_out = small_res[0, :, own]
        return top_out, grad_feat, outs[0], core_out, outs[1].transpose(0, 1, 3, 2), gate_out, bias_out, top_res

    dp = ('z', 'y', 'core')
    in_specs = (P(dp, 'tp'), P(dp, None), P(None, None, 'tp', None), P(), P(None, None, None, 'tp'), P(None, 'tp', None), P(None, 'tp'), P('tp', None))
    out_specs = (P(dp, None), P(dp, 'tp'), P(None, None, 'tp', None), P(), P(None, None, None, 'tp'), P(None, 'tp', None), P(None, 'tp'), P('tp', None))
    return jax.shard_map(device_body, mesh=mesh, in_specs=in_specs, out_specs=out_specs, check_vma=False)
```

```python
import jax
import jax.numpy as jnp
from jax import lax
from jax.experimental import pallas as pl
from jax.experimental.pallas import tpu as pltpu
from jax.sharding import Mesh, PartitionSpec as P

BF = jnp.bfloat16
F32 = jnp.float32
PLANE = ('z', 'y', 'core')


def cost(flops, nbytes):
    return pl.CostEstimate(flops=flops, bytes_accessed=nbytes, transcendentals=0)


def unpack_kernel(where_ref, local_ref, *refs):
    pieces, out_ref = refs[:-1], refs[-1]
    for i in range(len(pieces)):
        for j in range(4):
            @pl.when((pl.program_id(0) == i) & (pl.program_id(1) == j))
            def _():
                if j == 0:
                    out_ref[0] = local_ref[0]
                else:
                    out_ref[0] = pieces[i][j - 1].astype(BF)


def round_kernel(in_ref, out_ref):
    out_ref[...] = in_ref[...].astype(BF)


def round_low(values):
    return pl.pallas_call(round_kernel, out_shape=jax.ShapeDtypeStruct(values.shape, BF))(values)


def outer_kernel(left_ref, right_ref, out_ref):
    prod = lax.dot_general(left_ref[...], right_ref[0], (((1,), (1,)), ((), ())), preferred_element_type=F32)
    half = out_ref.shape[3]
    for h in range(2):
        out_ref[0, h, 0] = prod[h * half:(h + 1) * half]


def place_kernel(core_ref, mine_up, theirs_up, mine_down, theirs_down, *refs):
    down_ref, up_ref = refs[-2:]
    own = (pl.program_id(0) // 2 == core_ref[0])
    half = mine_up.shape[1]
    for h in range(2):
        down_ref[0, 0, h * half:(h + 1) * half] = jnp.where(own, mine_down[h], theirs_down[h])
        up_ref[0, 0, h * half:(h + 1) * half] = jnp.where(own, mine_up[h], theirs_up[h])


def solution(mesh):
    tp = mesh.shape['tp']
    mesh = Mesh(mesh.devices.reshape(tp, 4, 4, 2), ('tp', 'z', 'y', 'core'))

    def ring(axis, step):
        pairs = []
        for z in range(4):
            for y in range(4):
                for c in range(2):
                    along_y = (axis == 'a') == (c == 0)
                    to_z, to_y = (z, (y + step) % 4) if along_y else ((z + step) % 4, y)
                    pairs.append((z * 8 + y * 2 + c, to_z * 8 + to_y * 2 + c))
        return pairs

    def hop(values, axis, step):
        if axis == 'x':
            return lax.ppermute(values, 'tp', [(i, (i + step) % 4) for i in range(4)])
        return lax.ppermute(values, PLANE, ring(axis, step))

    def finite(values):
        return jnp.clip(values, jnp.finfo(F32).min, jnp.finfo(F32).max)

    def mm(spec, a, b):
        return jnp.einsum(spec, a, b, preferred_element_type=F32)

    def swap(values):
        return lax.ppermute(values, 'core', [(0, 1), (1, 0)])

    def flip(values):
        half = values.shape[-1] // 2
        return jnp.concatenate([values[..., half:], values[..., :half]], axis=-1)

    def both(part):
        return part + flip(swap(part))

    def device_body(feat_in, grad_out, w_down, w_core, w_up, w_gate, bias_cross, w_top):
        layers, experts, shard, rank = w_down.shape
        rows = feat_in.shape[0] // tp
        width = shard * tp
        heads = w_top.shape[1]
        own = experts // 2
        t = lax.axis_index('tp')
        core = lax.axis_index('core')
        z, y = lax.axis_index('z'), lax.axis_index('y')
        spot = {'x': t, 'a': jnp.where(core == 0, y, z), 'b': jnp.where(core == 0, z, y)}
        half = shard // 2
        first = core * own

        def gather(values, axis):
            cut = values.shape[-2] // 2
            back, ahead = hop(values, axis, 1), hop(values, axis, -1)
            far = jnp.concatenate([hop(back[..., :cut, :], axis, 1), hop(ahead[..., cut:, :], axis, -1)], axis=-2)
            return [values, ahead, far, back]

        def gather_way(values, axis, step):
            near, other = hop(values, axis, step), hop(values, axis, -step)
            far = hop(near, axis, step)
            return [values, other, far, near] if step == 1 else [values, near, far, other]

        def reduce_way(values, dim, axis, step):
            size = values.shape[dim] // 4

            def part(away):
                piece = lax.dynamic_slice_in_dim(values, (spot[axis] + away) % 4 * size, size, dim)
                return jnp.squeeze(piece, dim) if size == 1 else piece

            relay = hop(part(2 * step), axis, step)
            near = hop(part(-step), axis, -step)
            return part(0) + near + hop(part(step) + relay, axis, step)

        def ordered(pieces, axis, dim):
            shape = list(pieces[0].shape)
            size = shape[dim]
            shape[dim] = 4 * size
            out = jnp.zeros(shape, F32)
            for away, piece in enumerate(pieces):
                out = lax.dynamic_update_slice_in_dim(out, piece, ((spot[axis] + away) % 4) * size, dim)
            return out

        up_turned = w_up.transpose(0, 1, 3, 2)
        local = jnp.concatenate([lax.dynamic_slice(w_down, (0, first, 0, 0), (layers, own, shard, rank)),
                                 lax.dynamic_slice(up_turned, (0, first, 0, 0), (layers, own, shard, rank))], axis=1)
        pieces = lax.dynamic_index_in_dim(local, spot['a'], 1, keepdims=False)
        pieces = finite(pieces.astype(F32))
        small = jnp.concatenate([w_gate.transpose(0, 2, 1), bias_cross[:, None, :]], axis=1)
        small_count = layers * (experts + 1)
        small = finite(small.reshape(small_count, shard).astype(F32))
        small = jnp.pad(small, ((0, -small_count % 16), (0, rank - shard)))
        head = gather(jnp.concatenate([pieces[0], small], axis=0), 'x')
        small = ordered([part[None, shard:] for part in head], 'x', 0)
        small = small[:, :small_count, :shard].transpose(1, 0, 2).reshape(layers, experts + 1, width)
        queued = jnp.concatenate([pieces[1:], finite(w_top.astype(F32))[None]], axis=0)
        queued, head = lax.optimization_barrier((queued, head))
        others = gather(queued, 'x')[1:]
        stacks = [jnp.stack([part[:shard] for part in head[1:]])]
        stacks += [jnp.stack([part[n] for part in others]) for n in range(layers)]
        gathered = [gather(stack, 'a') for stack in stacks[:layers]]
        top_pieces = [stacks[layers]]
        where = jnp.stack([spot['a'], t]).astype(jnp.int32)

        send = finite(feat_in.T.astype(F32)).reshape(shard, tp, rows).transpose(1, 0, 2)
        got = lax.all_to_all(send, 'tp', 0, 0).reshape(width, rows)
        feat = jnp.concatenate([got, swap(got)], axis=1)
        gate_w = small[:, :experts].astype(BF)
        bias = small[:, experts]
        own_gate = lax.dynamic_slice(gate_w, (0, first, 0), (layers, own, width))
        own_core = lax.dynamic_slice(w_core, (0, first, 0, 0), (layers, own, rank, rank))
        grad_rows = lax.dynamic_slice(grad_out, (t * rows, 0), (rows, heads))
        grad_low = round_low(jnp.concatenate([grad_rows, swap(grad_rows)], axis=0))

        def matrices(local_part, parts):
            mats = local_part.shape[0]
            return pl.pallas_call(
                unpack_kernel,
                grid_spec=pltpu.PrefetchScalarGridSpec(
                    num_scalar_prefetch=1,
                    grid=(mats, tp),
                    in_specs=[pl.BlockSpec((1, shard, rank), lambda i, j, at: ((at[0] + i) % mats, 0, 0))]
                    + [pl.BlockSpec((3, shard, rank), lambda i, j, at: (0, 0, 0))] * len(parts),
                    out_specs=pl.BlockSpec((1, shard, rank), lambda i, j, at: ((at[0] + i) % mats, (at[1] + j) % 4, 0)),
                ),
                out_shape=jax.ShapeDtypeStruct((mats, width, rank), BF),
                cost_estimate=cost(2_000_000_000, 6 * mats * width * rank),
            )(where, local_part, *parts)

        def outer(left, right):
            out = pl.pallas_call(
                outer_kernel,
                grid=(own, tp),
                in_specs=[pl.BlockSpec((shard, left.shape[1]), lambda e, x: (x, 0)),
                          pl.BlockSpec((1, rank, left.shape[1]), lambda e, x: (e, 0, 0))],
                out_specs=pl.BlockSpec((1, 2, 1, half, rank), lambda e, x: (e, 0, x, 0, 0)),
                out_shape=jax.ShapeDtypeStruct((own, 2, tp, half, rank), F32),
                cost_estimate=cost(2 * own * rank * width * left.shape[1], 4 * own * rank * width),
            )(left, right)
            return out.reshape(2 * own, tp, half, rank)

        weights, saved = [], []
        state = feat.astype(BF)
        for layer in range(layers):
            parts = gathered[layer]
            early = [(layer + 1, k) for k in (0, 1, 3)] + [(layer + 2, 0)]
            early = [(n, k) for n, k in early if n < layers]
            parts, state, tied = lax.optimization_barrier((parts, state, [gathered[n][k] for n, k in early]))
            for (n, k), value in zip(early, tied):
                gathered[n][k] = value
            w_all = matrices(local[layer], parts)
            down_w, up_t = w_all[:own], w_all[own:]
            weights.append((down_w, up_t))
            act_one = jnp.tanh(mm('ewr,wn->ern', down_w, state))
            gate = jax.nn.softmax(mm('ew,wn->en', gate_w[layer], state), axis=0)
            own_share = lax.dynamic_slice(gate, (first, 0), (own, gate.shape[1]))[:, None, :]
            act_low = act_one.astype(BF)
            act_two = jnp.tanh(mm('ers,ern->esn', own_core[layer], act_low))
            mixed = (own_share * act_two).astype(BF)
            mix_bias = both(mm('ewr,ern->wn', up_t, mixed)) + bias[layer][:, None]
            saved.append((state, act_one, act_low, act_two, own_share, mixed, mix_bias))
            state = (state.astype(F32) + feat * mix_bias).astype(BF)
        top_w = matrices(w_top[None], top_pieces)[0]
        top_rows = mm('wn,wh->nh', state[:, :rows], top_w)
        top_out = jnp.zeros((tp, rows, heads), F32)
        top_out = lax.dynamic_update_slice(top_out, top_rows[None], (t, 0, 0))
        for shift in range(1, tp):
            part = lax.ppermute(top_rows, 'tp', [(i, (i + shift) % tp) for i in range(tp)])
            top_out = lax.dynamic_update_slice(top_out, part[None], ((t - shift) % tp, 0, 0))
        top_out = top_out.reshape(tp * rows, heads)

        grad_state = mm('wh,nh->wn', top_w, grad_low)
        own_state = lax.dynamic_slice(state.reshape(tp, shard, -1), (0, core * half, 0), (tp, half, state.shape[1]))
        grad_top = mm('xwn,nh->xwh', own_state, grad_low)
        grad_feat = jnp.zeros((width, rows), F32)
        reduced = [None] * layers

        def reduce_pair(up_blocks, down_blocks, layer):
            if layer == layers - 1:
                pair = [reduce_way(up_blocks, 1, 'x', 1), reduce_way(down_blocks, 1, 'x', -1)]
            else:
                pair = [reduce_way(up_blocks, 0, 'a', 1), reduce_way(down_blocks, 0, 'a', -1)]
            return pair

        def reduce_more(pair, layer):
            pair = jnp.concatenate(pair, axis=1)
            return reduce_way(pair, 0, 'a' if layer == layers - 1 else 'x', 1 if layer % 2 else -1)

        def all_b(part, step):
            part = reduce_way(part, 1, 'b', step)
            return ordered(gather_way(part, 'b', step), 'b', 1)

        def all_a(part):
            return ordered([piece[None] for piece in gather(part, 'a')], 'a', 0)

        core_grads, small_grads = [None] * layers, [None] * layers
        outs = None
        core_id = core.astype(jnp.int32).reshape(1)
        for layer in reversed(range(layers)):
            state_in, act_one, act_low, act_two, own_share, mixed, mix_bias = saved[layer]
            down_w, up_t = weights[layer]
            grad_feat = grad_feat + grad_state[:, :rows] * mix_bias[:, :rows]
            grad_mix = grad_state * feat
            grad_bias = jnp.sum(grad_mix, axis=1)
            grad_mix_low = grad_mix.astype(BF)
            blocks, grad_mix_low = lax.optimization_barrier((outer(grad_mix_low, mixed), grad_mix_low))
            up_blocks = blocks
            grad_mixed = mm('ewr,wn->ern', up_t, grad_mix_low)
            gate_act = jnp.sum(grad_mixed * act_two, axis=1)
            grad_mid = (grad_mixed * own_share * (1.0 - act_two * act_two)).astype(BF)
            core_grads[layer] = mm('ern,esn->ers', act_low, grad_mid)
            grad_act = mm('ers,esn->ern', own_core[layer], grad_mid)
            grad_proj = (grad_act * (1.0 - act_one * act_one)).astype(BF)
            blocks, grad_proj = lax.optimization_barrier((outer(state_in, grad_proj), grad_proj))
            if layer == 0:
                blocks, reduced[1:] = lax.optimization_barrier((blocks, reduced[1:]))
            reduced[layer] = reduce_pair(up_blocks, blocks, layer)
            share = own_share[:, 0]
            total = both(jnp.sum(share * gate_act, axis=0, keepdims=True))
            grad_logit = (share * (gate_act - total)).astype(BF)
            grad_gate = mm('en,wn->ew', grad_logit, state_in)
            small_grads[layer] = jnp.concatenate([grad_gate, grad_bias[None]], axis=0)
            part = mm('ewr,ern->wn', down_w, grad_proj) + mm('ew,en->wn', own_gate[layer], grad_logit)
            grad_state = grad_state + both(part)
        grad_feat = grad_feat + grad_state[:, :rows]
        grad_feat = lax.all_to_all(grad_feat.reshape(tp, shard, rows), 'tp', 0, 0)
        grad_feat = grad_feat.transpose(1, 0, 2).reshape(shard, tp * rows).T

        def place(outs, mine, theirs, layer, up_slot):
            spots = [pl.BlockSpec((2, half, rank), lambda e, n=n: (e % own, n, 0)) for n in (up_slot, up_slot, up_slot + 1, up_slot + 1)]
            target = pl.BlockSpec((1, 1, shard, rank), lambda e: (layer, e, 0, 0))
            return pl.pallas_call(
                place_kernel,
                grid=(experts,),
                in_specs=[pl.BlockSpec(memory_space=pltpu.SMEM)] + spots + [pl.BlockSpec(memory_space=pl.ANY)] * (2 if outs else 0),
                out_specs=[target, target],
                out_shape=[jax.ShapeDtypeStruct((layers, experts, shard, rank), F32)] * 2,
                input_output_aliases={5: 0, 6: 1} if outs else {},
                cost_estimate=cost(2_000_000_000, 24 * experts * shard * rank),
            )(core_id, mine, theirs, mine, theirs, *(outs or ()))

        upper = list(reversed(range(1, layers)))
        mine_upper = all_a(all_b(jnp.concatenate([reduce_more(reduced[layer], layer) for layer in upper], axis=0), -1))
        theirs_upper = swap(mine_upper)

        lanes = rank
        small_rows = layers * (own + 1)
        core_all = jnp.stack(core_grads).reshape(4, tp, -1, lanes)
        core_len = core_all.shape[2]
        pad_rows = -half % 32
        top_cut = jnp.pad(grad_top, ((0, 0), (0, pad_rows), (0, 0))).reshape(tp, 4, -1, lanes).transpose(1, 0, 2, 3)
        top_len = top_cut.shape[2]
        small_cut = jnp.stack(small_grads).reshape(small_rows, tp, shard).transpose(1, 0, 2)
        small_cut = jnp.pad(small_cut, ((0, 0), (0, 16 - small_rows), (0, lanes - shard)))
        small_cut = small_cut.reshape(tp, 4, 4, lanes).transpose(1, 0, 2, 3)
        small_cut = jnp.pad(small_cut, ((0, 0), (0, 0), (0, -(core_len + top_len + 4) % 16), (0, 0)))
        misc = jnp.concatenate([core_all, top_cut, small_cut], axis=2)
        cut = misc.shape[2] // 2
        last = [reduce_way(part, 0, 'x', step) for part, step in zip(reduced[0], (1, -1))]
        last += [reduce_way(reduce_way(part, 1, 'x', step), 0, 'a', step) for part, step in ((misc[:, :, :cut], 1), (misc[:, :, cut:], -1))]
        last = all_b(jnp.concatenate(last, axis=0), 1)
        grad_feat, top_out, last = lax.optimization_barrier((grad_feat, top_out, last))
        cores = ordered(gather_way(last[shard:shard + core_len], 'x', 1), 'x', 0)
        joined = jnp.concatenate([last[:shard], cores, last[shard + core_len:]], axis=0)
        joined, mine_upper, theirs_upper = lax.optimization_barrier((joined, mine_upper, theirs_upper))
        mine = all_a(joined)
        theirs = swap(mine)
        for n, layer in enumerate(upper):
            outs = place(outs, mine_upper, theirs_upper, layer, 2 * n)
        outs = place(outs, mine, theirs, 0, 0)

        def paired(values, other, axis):
            return jnp.where(core == 0, jnp.concatenate([values, other], axis=axis), jnp.concatenate([other, values], axis=axis))

        both_cores = [values[:, shard:shard + tp * core_len].reshape(layers, own, rank, rank) for values in (mine, theirs)]
        core_out = paired(*both_cores, 1)
        rest = paired(*[values[None, :, shard + tp * core_len:] for values in (mine, theirs)], 0)
        top_res = rest[:, :, :top_len].reshape(2, half + pad_rows, heads)[:, :half].reshape(shard, heads)
        small_res = rest[:, :, top_len:top_len + 4, :shard].reshape(2, 16, shard)[:, :small_rows].reshape(2, layers, own + 1, shard)
        gate_out = small_res[:, :, :own].transpose(1, 3, 0, 2).reshape(layers, shard, experts)
        bias_out = small_res[0, :, own]
        return top_out, grad_feat, outs[0], core_out, outs[1].transpose(0, 1, 3, 2), gate_out, bias_out, top_res

    dp = ('z', 'y', 'core')
    in_specs = (P(dp, 'tp'), P(dp, None), P(None, None, 'tp', None), P(), P(None, None, None, 'tp'), P(None, 'tp', None), P(None, 'tp'), P('tp', None))
    out_specs = (P(dp, None), P(dp, 'tp'), P(None, None, 'tp', None), P(), P(None, None, None, 'tp'), P(None, 'tp', None), P(None, 'tp'), P('tp', None))
    return jax.shard_map(device_body, mesh=mesh, in_specs=in_specs, out_specs=out_specs, check_vma=False)
```
